32 devices in a mesh: scan: 2 (over y), ang: 4 (over z), row: 4 (over x, core).
Axes of the slice: x: 2, y: 2, z: 4, core: 2. Of those that a mesh axis runs over, the one named last changes fastest.
Arguments:
- projections: bfloat16 [8, 32, 2560], P(('scan', 'ang'), 'row'), parts along dimension 0, may hold values from 0 to 2
- flats: float32 [64, 2560], P(('scan', 'row')), parts along dimension 0, may hold values from 1 to 3
- block_start: int32 [4, 4], replicated, may hold values from 0 to 2528
- bp_weights: bfloat16 [4, 32, 1024], P(None, None, 'ang'), may hold values from -0.5 to 0.5
Outputs:
- recon: float32 [64, 1024], P(('scan', 'row'), 'ang'), parts along dimension 0
The draws below stay inside these ranges and needn't reach their ends.
There are 2 independent parts, one for each index of `scan`. The reference program is written for one: setup_inputs(seed, part) draws one part's arguments, and reference() takes and returns one part's arrays. A program takes and returns all parts, laid end to end along the dimension named above; an argument that names none is the same for every part. Nothing has to cross between parts.
Inputs may be any that keep to these rules, and one draw needn't show every extreme that they name: block_start[a, r] is the first of the 32 detector columns that pixel region r reads at angle a.
All inputs are finite; a program needn't handle non-finite values.
Results may differ from the reference program's by a relative error of at most 0.009.
Values may be sent and summed in bfloat16 or wider, within the bound.
A program may use at most 64 MiB of HBM per device.

```python
import math
import jax
import jax.numpy as jnp
from jax import lax

W = 2560
RD = 8
HALO = 4
CB = 32
PIX_DEV = 256
TILE = 16
ANGLES = 4
SLICES = 32
REGIONS = 4
PIX = 1024


def set_ends(entries, stream_key, smallest, largest):
    shape = entries.shape
    spot = [jax.random.randint(jax.random.fold_in(stream_key, axis), (), 0, shape[axis]) for axis in range(len(shape))]
    entries = entries.at[tuple(spot)].set(smallest)
    longest = shape.index(max(shape))
    spot[longest] = (spot[longest] + 1) % shape[longest]
    return entries.at[tuple(spot)].set(largest)


def levels(rng, extent, shards, least, largest):
    factor_of = 1.0
    for position, shards_of in shards:
        steps = jax.random.uniform(jax.random.fold_in(jax.random.fold_in(rng, 6), position), (shards_of,), jnp.float32, least / len(shards), largest / len(shards))
        factor_of = factor_of * jnp.repeat(jnp.exp(steps), extent[position] // shards_of).reshape((-1,) + (1,) * (len(extent) - 1 - position))
    return factor_of


def gaussian(own_key, dims, scale, bound, shards=(), kind=jnp.bfloat16):
    array = jax.random.normal(own_key, dims, jnp.float32) * scale
    if len(shards) > 0:
        array = levels(own_key, dims, shards, -0.22, 0.18) * array
    return jnp.clip(array, min=-bound, max=bound).astype(kind)


def setup_inputs(seed: int = 0, part: int = 0) -> dict:
    keys = jax.random.split(jax.random.key(seed), 5)
    part_splits = jax.random.split(jax.random.fold_in(keys[4], part), 5)
    projections = jnp.clip(2.0 * jax.random.uniform(part_splits[0], (ANGLES, SLICES, W), jnp.float32) ** levels(part_splits[0], (ANGLES, SLICES, W), ((0, 4), (1, 4)), -0.2, 0.2), 0.0, 2.0).astype(jnp.bfloat16)
    flats = jnp.clip(jnp.exp(math.log(3.0) - 1.0986123 * jax.random.uniform(part_splits[1], (SLICES, W), jnp.float32) ** levels(part_splits[1], (SLICES, W), ((0, 4),), -0.2, 0.2)), 1.0, 3.0)
    block_start = set_ends(jax.random.randint(keys[2], (ANGLES, REGIONS), 0, W - CB + 1), jax.random.fold_in(keys[2], 1), 0, W - CB).astype(jnp.int32)
    bp_weights = gaussian(keys[3], (ANGLES, CB, PIX), (ANGLES * CB) ** -0.5, 0.5, ((2, 4),))
    return dict(projections=projections, flats=flats, block_start=block_start, bp_weights=bp_weights)


paganin_beta = 8.0
ramp_gain = 320.0


def reference(projections, flats, block_start, bp_weights):
    contrast = 1.0 - projections.astype(jnp.float32) / flats[None, :, :]
    padded = jnp.pad(contrast, ((0, 0), (HALO, HALO), (0, 0)))
    tile_count = SLICES // RD
    row_index = (jnp.arange(tile_count, dtype=jnp.int32)[:, None] * RD
                 + jnp.arange(TILE, dtype=jnp.int32)[None, :]).astype(jnp.int32)
    row_freq = jnp.arange(TILE, dtype=jnp.float32)
    col_freq = jnp.arange(W, dtype=jnp.float32)
    lam = (4.0 * jnp.sin(jnp.pi * row_freq / TILE) ** 2)[:, None] + (4.0 * jnp.sin(jnp.pi * col_freq / W) ** 2)[None, :]
    filt = 1.0 / (1.0 + paganin_beta * lam)
    folded = jnp.minimum(col_freq, W - col_freq)
    ramp = ramp_gain * (folded / W) * (0.5 + 0.5 * jnp.cos(2.0 * jnp.pi * folded / W))

    def one_angle(angle_rows):
        tiles = angle_rows[row_index]
        spectrum = jnp.fft.fft2(tiles, axes=(1, 2)) * filt
        back = jnp.real(jnp.fft.ifft2(spectrum, axes=(1, 2)))
        paganin = back[:, HALO:HALO + RD, :].reshape(SLICES, W)
        filtered = jnp.real(jnp.fft.ifft(jnp.fft.fft(paganin, axis=-1) * ramp, axis=-1))
        return filtered.astype(jnp.bfloat16)

    sinogram = lax.map(one_angle, padded)
    offsets = jnp.arange(CB, dtype=jnp.int32)

    def one_region(region):
        starts = lax.dynamic_index_in_dim(block_start, region, 1, keepdims=False)
        index = (starts[:, None] + offsets[None, :]).astype(jnp.int32)
        index = jnp.broadcast_to(index[:, None, :], (ANGLES, SLICES, CB))
        blocks = jnp.take_along_axis(sinogram, index, axis=2)
        weights = lax.dynamic_slice_in_dim(bp_weights, region * PIX_DEV, PIX_DEV, 2)
        return jnp.einsum('asc,acp->sp', blocks.astype(jnp.float32), weights.astype(jnp.float32))

    parts = lax.map(one_region, jnp.arange(REGIONS, dtype=jnp.int32))
    return jnp.transpose(parts, (1, 0, 2)).reshape(SLICES, PIX)
```

```python
import functools

import jax
import jax.numpy as jnp
import numpy as np
from jax import lax
from jax.experimental import pallas as pl
from jax.experimental.pallas import tpu as pltpu
from jax.sharding import PartitionSpec as P

HALO = 4
LANES = 128
CHUNK = 512
paganin_beta = 8.0
ramp_gain = 320.0


def filter_table(tile_rows, width, cb_width):
    u = np.arange(tile_rows, dtype=np.float64)
    v = np.arange(width, dtype=np.float64)
    lam = (4.0 * np.sin(np.pi * u / tile_rows) ** 2)[:, None] + (4.0 * np.sin(np.pi * v / width) ** 2)[None, :]
    folded = np.minimum(v, width - v)
    ramp = ramp_gain * (folded / width) * (0.5 + 0.5 * np.cos(2.0 * np.pi * folded / width))
    taps = np.real(np.fft.ifft2(ramp[None, :] / (1.0 + paganin_beta * lam)))
    lags = tile_rows // 2 + 1
    place = (np.arange(cb_width)[:, None] - np.arange(width)[None, :]) % width
    table = taps[:lags][:, place].reshape(lags * cb_width, width)
    chunks = width // CHUNK
    return table.reshape(lags * cb_width, chunks, CHUNK).transpose(1, 0, 2)


def kernel(regions, tiles, starts, proj, flats, table, weights, out,
           starts_s, proj_v, flats_v, table_v, weights_v, xs, ys, sbuf, rbuf, out_v,
           load_sem, table_sem, out_sem, send_sem, recv_sem):
    rows, width = flats.shape
    blocks = width // LANES
    chunks = table.shape[0]
    angles, cb, _ = weights.shape
    per = LANES // cb
    half = rows // 2
    me = lax.axis_index("ang")
    row = lax.axis_index("row")

    def peer(step, delta):
        return {"ang": lax.rem(me + step, regions), "row": lax.rem(row + delta + tiles, tiles)}

    links = [(step, delta) for step in range(regions) for delta in (-1, 0, 1) if (step, delta) != (0, 0)]
    barrier = pltpu.get_barrier_semaphore()
    for step, delta in links:
        pl.semaphore_signal(barrier, inc=1, device_id=peer(step, delta), device_id_type=pl.DeviceIdType.MESH)

    loads = [pltpu.make_async_copy(proj.at[0], proj_v, load_sem.at[0]),
             pltpu.make_async_copy(flats, flats_v, load_sem.at[1]),
             pltpu.make_async_copy(starts, starts_s, load_sem.at[3])]
    late = [pltpu.make_async_copy(table.at[k], table_v.at[k], table_sem.at[k]) for k in range(chunks)]
    weight_load = pltpu.make_async_copy(weights, weights_v, load_sem.at[2])
    for copy in loads + late + [weight_load]:
        copy.start()
    for copy in loads:
        copy.wait()

    pieces = [slice(b * LANES, (b + 1) * LANES) for b in range(blocks)]
    contrast = [1.0 - proj_v[:, p].astype(jnp.float32) / flats_v[:, p] for p in pieces]
    mean = jnp.sum(sum(contrast), axis=1, keepdims=True) / width
    for b, x in enumerate(contrast):
        xs[b] = x - mean
        xs[b + blocks] = x - mean

    lane = lax.broadcasted_iota(jnp.int32, (rows, LANES), 1)
    sub = lax.broadcasted_iota(jnp.int32, (rows, LANES), 0)
    for g in range(regions):
        start = starts_s[me, g]
        first = start // LANES
        rest = lax.rem(start, LANES)
        shift = lax.rem(LANES - rest, LANES)
        low = lane < LANES - rest
        left = pltpu.roll(xs[first], shift, 1)
        for b in range(blocks):
            right = pltpu.roll(xs[first + b + 1], shift, 1)
            y = jnp.where(low, left, right)
            high = y.astype(jnp.bfloat16).astype(jnp.float32)
            pair = jnp.concatenate([high, y - high], axis=0).astype(jnp.bfloat16)
            ys[g * 2 * rows:(g + 1) * 2 * rows, b * LANES:(b + 1) * LANES] = pair
            left = right

    total = None
    for k in range(chunks):
        late[k].wait()
        part = lax.dot_general(ys[:, k * CHUNK:(k + 1) * CHUNK], table_v[k], (((1,), (1,)), ((), ())),
                               preferred_element_type=jnp.float32)
        total = part if total is None else total + part

    lags = rows + 1
    pad = -(lags * cb) % LANES
    total = jnp.concatenate([total, jnp.zeros((total.shape[0], pad), jnp.float32)], axis=1)
    spot = lax.rem(me, per) * cb
    mine = (lane >= spot) & (lane < spot + cb)
    for g in range(regions):
        pg = total[g * 2 * rows:g * 2 * rows + rows] + total[g * 2 * rows + rows:(g + 1) * 2 * rows]
        lag = []
        for d in range(lags):
            tile = pg[:, d // per * LANES:(d // per + 1) * LANES]
            lag.append(pltpu.roll(tile, lax.rem(spot + LANES - d % per * cb, LANES), 1))
        own = lag[0]
        after = jnp.where(sub >= half, lag[rows], 0.0)
        before = jnp.where(sub < half, lag[rows], 0.0)
        for e in range(1, rows):
            a = pltpu.roll(lag[e], e, 0)
            b = pltpu.roll(lag[rows - e], e, 0)
            own = own + jnp.where(sub >= e, a, b)
            other = jnp.where(sub >= e, b, a)
            source = lax.rem(sub + rows - e, rows)
            after = after + jnp.where(source >= half, other, 0.0)
            before = before + jnp.where(source < half, other, 0.0)
        sbuf[0, g] = jnp.where(mine, before, 0.0).astype(jnp.bfloat16)
        sbuf[1, g] = jnp.where(mine, own, 0.0).astype(jnp.bfloat16)
        sbuf[2, g] = jnp.where(mine, after, 0.0).astype(jnp.bfloat16)

    pl.semaphore_wait(barrier, len(links))

    def message(step, delta):
        to = peer(step, delta)
        region = to["ang"]
        return pltpu.make_async_remote_copy(
            src_ref=sbuf.at[delta + 1, region], dst_ref=rbuf.at[delta + 1, me],
            send_sem=send_sem.at[delta + 1, region], recv_sem=recv_sem.at[delta + 1, me],
            device_id=to, device_id_type=pl.DeviceIdType.MESH)

    sent = [message(step, delta) for step, delta in links]
    for copy in sent:
        copy.start()
    weight_load.wait()

    def arrived(step, delta):
        angle = lax.rem(me + step, regions)
        pltpu.make_async_remote_copy(
            src_ref=sbuf.at[delta + 1, angle], dst_ref=rbuf.at[delta + 1, angle],
            send_sem=send_sem.at[delta + 1, angle], recv_sem=recv_sem.at[delta + 1, angle],
            device_id=peer(step, delta), device_id_type=pl.DeviceIdType.MESH).wait_recv()

    rbuf[1, me] = sbuf[1, me]
    for step, delta in links:
        arrived(step, delta)

    result = jnp.zeros(out.shape, jnp.float32)
    for group in range(-(-angles // per)):
        block = jnp.zeros((rows, LANES), jnp.float32)
        members = range(group * per, min(angles, (group + 1) * per))
        for a in members:
            block = block + rbuf[1, a].astype(jnp.float32)
            block = block + jnp.where(row < tiles - 1, rbuf[0, a].astype(jnp.float32), 0.0)
            block = block + jnp.where(row > 0, rbuf[2, a].astype(jnp.float32), 0.0)
        block = block.astype(jnp.bfloat16)
        depth = len(members) * cb
        w = weights_v[group * per:group * per + len(members)].reshape(depth, out.shape[1])
        result = result + jnp.dot(block[:, :depth], w, preferred_element_type=jnp.float32)
    out_v[...] = result
    store = pltpu.make_async_copy(out_v, out, out_sem)
    store.start()
    for copy in sent:
        copy.wait_send()
    store.wait()


def body(projections, flats, block_start, bp_weights):
    _, rows, width = projections.shape
    angles, cb, pixels = bp_weights.shape
    regions, tiles = lax.axis_size("ang"), lax.axis_size("row")
    table = jnp.asarray(filter_table(rows + 2 * HALO, width, cb), jnp.bfloat16)
    hbm = pl.BlockSpec(memory_space=pl.ANY)
    return pl.pallas_call(
        functools.partial(kernel, regions, tiles),
        name="fbp",
        out_shape=jax.ShapeDtypeStruct((rows, pixels), jnp.float32),
        in_specs=[hbm, hbm, hbm, hbm, hbm],
        out_specs=hbm,
        scratch_shapes=[
            pltpu.SMEM(block_start.shape, jnp.int32),
            pltpu.VMEM((rows, width), jnp.bfloat16),
            pltpu.VMEM((rows, width), jnp.float32),
            pltpu.VMEM(table.shape, jnp.bfloat16),
            pltpu.VMEM(bp_weights.shape, jnp.bfloat16),
            pltpu.VMEM((2 * width // LANES, rows, LANES), jnp.float32),
            pltpu.VMEM((regions * 2 * rows, width), jnp.bfloat16),
            pltpu.VMEM((3, regions, rows, LANES), jnp.bfloat16),
            pltpu.VMEM((3, angles, rows, LANES), jnp.bfloat16),
            pltpu.VMEM((rows, pixels), jnp.float32),
            pltpu.SemaphoreType.DMA((4,)),
            pltpu.SemaphoreType.DMA((table.shape[0],)),
            pltpu.SemaphoreType.DMA,
            pltpu.SemaphoreType.DMA((3, regions)),
            pltpu.SemaphoreType.DMA((3, angles)),
        ],
        compiler_params=pltpu.CompilerParams(collective_id=0, has_side_effects=True),
    )(block_start, projections, flats, table, bp_weights)


def solution(mesh):
    placed = (P(("scan", "ang"), "row", None), P(("scan", "row"), None), P(), P(None, None, "ang"))
    return jax.shard_map(
        body, mesh=mesh, in_specs=placed, out_specs=P(("scan", "row"), "ang"), check_vma=False
    )
```

```python
import functools

import jax
import jax.numpy as jnp
import numpy as np
from jax import lax
from jax.experimental import pallas as pl
from jax.experimental.pallas import tpu as pltpu
from jax.sharding import PartitionSpec as P

HALO = 4
LANES = 128
CHUNK = 512
paganin_beta = 8.0
ramp_gain = 320.0


def filter_table(tile_rows, width, cb_width):
    u = np.arange(tile_rows, dtype=np.float64)
    v = np.arange(width, dtype=np.float64)
    lam = (4.0 * np.sin(np.pi * u / tile_rows) ** 2)[:, None] + (4.0 * np.sin(np.pi * v / width) ** 2)[None, :]
    folded = np.minimum(v, width - v)
    ramp = ramp_gain * (folded / width) * (0.5 + 0.5 * np.cos(2.0 * np.pi * folded / width))
    taps = np.real(np.fft.ifft2(ramp[None, :] / (1.0 + paganin_beta * lam)))
    lags = tile_rows // 2 + 1
    place = (np.arange(cb_width)[:, None] - np.arange(width)[None, :]) % width
    table = taps[:lags][:, place].reshape(lags * cb_width, width)
    chunks = width // CHUNK
    return table.reshape(lags * cb_width, chunks, CHUNK).transpose(1, 0, 2)


def kernel(regions, tiles, starts, proj, flats, table, weights, out,
           starts_s, proj_v, flats_v, table_v, weights_v, xs, ys, sbuf, rbuf,
           load_sem, table_sem, send_sem, recv_sem):
    rows, width = flats.shape
    blocks = width // LANES
    chunks = table.shape[0]
    angles, cb, _ = weights.shape
    per = LANES // cb
    half = rows // 2
    me = lax.axis_index("ang")
    row = lax.axis_index("row")

    def peer(step, delta):
        return {"ang": lax.rem(me + step, regions), "row": lax.rem(row + delta + tiles, tiles)}

    links = [(step, delta) for step in range(regions) for delta in (-1, 0, 1) if (step, delta) != (0, 0)]
    barrier = pltpu.get_barrier_semaphore()
    for step, delta in links:
        pl.semaphore_signal(barrier, inc=1, device_id=peer(step, delta), device_id_type=pl.DeviceIdType.MESH)

    loads = [pltpu.make_async_copy(proj.at[0], proj_v, load_sem.at[0]),
             pltpu.make_async_copy(flats, flats_v, load_sem.at[1]),
             pltpu.make_async_copy(starts, starts_s, load_sem.at[3])]
    late = [pltpu.make_async_copy(table.at[k], table_v.at[k], table_sem.at[k]) for k in range(chunks)]
    weight_load = pltpu.make_async_copy(weights, weights_v, load_sem.at[2])
    for copy in loads + late + [weight_load]:
        copy.start()
    for copy in loads:
        copy.wait()

    pieces = [slice(b * LANES, (b + 1) * LANES) for b in range(blocks)]
    contrast = [1.0 - proj_v[:, p].astype(jnp.float32) / flats_v[:, p] for p in pieces]
    mean = jnp.sum(sum(contrast), axis=1, keepdims=True) / width
    for b, x in enumerate(contrast):
        xs[b] = x - mean
        xs[b + blocks] = x - mean

    lane = lax.broadcasted_iota(jnp.int32, (rows, LANES), 1)
    sub = lax.broadcasted_iota(jnp.int32, (rows, LANES), 0)
    for g in range(regions):
        start = starts_s[me, g]
        first = start // LANES
        rest = lax.rem(start, LANES)
        shift = lax.rem(LANES - rest, LANES)
        low = lane < LANES - rest
        left = pltpu.roll(xs[first], shift, 1)
        for b in range(blocks):
            right = pltpu.roll(xs[first + b + 1], shift, 1)
            y = jnp.where(low, left, right)
            high = y.astype(jnp.bfloat16).astype(jnp.float32)
            pair = jnp.concatenate([high, y - high], axis=0).astype(jnp.bfloat16)
            ys[g * 2 * rows:(g + 1) * 2 * rows, b * LANES:(b + 1) * LANES] = pair
            left = right

    total = None
    for k in range(chunks):
        late[k].wait()
        part = lax.dot_general(ys[:, k * CHUNK:(k + 1) * CHUNK], table_v[k], (((1,), (1,)), ((), ())),
                               preferred_element_type=jnp.float32)
        total = part if total is None else total + part

    lags = rows + 1
    pad = -(lags * cb) % LANES
    total = jnp.concatenate([total, jnp.zeros((total.shape[0], pad), jnp.float32)], axis=1)
    spot = lax.rem(me, per) * cb
    mine = (lane >= spot) & (lane < spot + cb)
    for g in range(regions):
        pg = total[g * 2 * rows:g * 2 * rows + rows] + total[g * 2 * rows + rows:(g + 1) * 2 * rows]
        lag = []
        for d in range(lags):
            tile = pg[:, d // per * LANES:(d // per + 1) * LANES]
            lag.append(pltpu.roll(tile, lax.rem(spot + LANES - d % per * cb, LANES), 1))
        own = lag[0]
        after = jnp.where(sub >= half, lag[rows], 0.0)
        before = jnp.where(sub < half, lag[rows], 0.0)
        for e in range(1, rows):
            a = pltpu.roll(lag[e], e, 0)
            b = pltpu.roll(lag[rows - e], e, 0)
            own = own + jnp.where(sub >= e, a, b)
            other = jnp.where(sub >= e, b, a)
            source = lax.rem(sub + rows - e, rows)
            after = after + jnp.where(source >= half, other, 0.0)
            before = before + jnp.where(source < half, other, 0.0)
        sbuf[0, g] = jnp.where(mine, before, 0.0).astype(jnp.bfloat16)
        sbuf[1, g] = jnp.where(mine, own, 0.0).astype(jnp.bfloat16)
        sbuf[2, g] = jnp.where(mine, after, 0.0).astype(jnp.bfloat16)

    pl.semaphore_wait(barrier, len(links))

    def message(step, delta):
        to = peer(step, delta)
        region = to["ang"]
        return pltpu.make_async_remote_copy(
            src_ref=sbuf.at[delta + 1, region], dst_ref=rbuf.at[delta + 1, me],
            send_sem=send_sem.at[delta + 1, region], recv_sem=recv_sem.at[delta + 1, me],
            device_id=to, device_id_type=pl.DeviceIdType.MESH)

    sent = [message(step, delta) for step, delta in links]
    for copy in sent:
        copy.start()
    weight_load.wait()

    def arrived(step, delta):
        angle = lax.rem(me + step, regions)
        pltpu.make_async_remote_copy(
            src_ref=sbuf.at[delta + 1, angle], dst_ref=rbuf.at[delta + 1, angle],
            send_sem=send_sem.at[delta + 1, angle], recv_sem=recv_sem.at[delta + 1, angle],
            device_id=peer(step, delta), device_id_type=pl.DeviceIdType.MESH).wait_recv()

    rbuf[1, me] = sbuf[1, me]
    for step, delta in links:
        arrived(step, delta)

    result = jnp.zeros(out.shape, jnp.float32)
    for group in range(-(-angles // per)):
        block = jnp.zeros((rows, LANES), jnp.float32)
        members = range(group * per, min(angles, (group + 1) * per))
        for a in members:
            block = block + rbuf[1, a].astype(jnp.float32)
            block = block + jnp.where(row < tiles - 1, rbuf[0, a].astype(jnp.float32), 0.0)
            block = block + jnp.where(row > 0, rbuf[2, a].astype(jnp.float32), 0.0)
        block = block.astype(jnp.bfloat16)
        depth = len(members) * cb
        w = weights_v[group * per:group * per + len(members)].reshape(depth, out.shape[1])
        result = result + jnp.dot(block[:, :depth], w, preferred_element_type=jnp.float32)
    out[...] = result
    for copy in sent:
        copy.wait_send()


def body(projections, flats, block_start, bp_weights):
    _, rows, width = projections.shape
    angles, cb, pixels = bp_weights.shape
    regions, tiles = lax.axis_size("ang"), lax.axis_size("row")
    table = jnp.asarray(filter_table(rows + 2 * HALO, width, cb), jnp.bfloat16)
    hbm = pl.BlockSpec(memory_space=pltpu.HBM)
    return pl.pallas_call(
        functools.partial(kernel, regions, tiles),
        name="fbp",
        out_shape=pltpu.VMEM((rows, pixels), jnp.float32),
        in_specs=[hbm, hbm, hbm, hbm, hbm],
        out_specs=pl.BlockSpec(memory_space=pltpu.VMEM),
        scratch_shapes=[
            pltpu.SMEM(block_start.shape, jnp.int32),
            pltpu.VMEM((rows, width), jnp.bfloat16),
            pltpu.VMEM((rows, width), jnp.float32),
            pltpu.VMEM(table.shape, jnp.bfloat16),
            pltpu.VMEM(bp_weights.shape, jnp.bfloat16),
            pltpu.VMEM((2 * width // LANES, rows, LANES), jnp.float32),
            pltpu.VMEM((regions * 2 * rows, width), jnp.bfloat16),
            pltpu.VMEM((3, regions, rows, LANES), jnp.bfloat16),
            pltpu.VMEM((3, angles, rows, LANES), jnp.bfloat16),
            pltpu.SemaphoreType.DMA((4,)),
            pltpu.SemaphoreType.DMA((table.shape[0],)),
            pltpu.SemaphoreType.DMA((3, regions)),
            pltpu.SemaphoreType.DMA((3, angles)),
        ],
        compiler_params=pltpu.CompilerParams(collective_id=0, has_side_effects=True, vmem_limit_bytes=65000000),
    )(block_start, projections, flats, table, bp_weights)


def solution(mesh):
    placed = (P(("scan", "ang"), "row", None), P(("scan", "row"), None), P(), P(None, None, "ang"))
    return jax.shard_map(
        body, mesh=mesh, in_specs=placed, out_specs=P(("scan", "row"), "ang"), check_vma=False
    )
```

```python
import functools

import jax
import jax.numpy as jnp
import numpy as np
from jax import lax
from jax.experimental import pallas as pl
from jax.experimental.pallas import tpu as pltpu
from jax.sharding import PartitionSpec as P

HALO = 4
LANES = 128
CHUNK = 512
SHIFTS = 2
paganin_beta = 8.0
ramp_gain = 320.0


def filter_table(tile_rows, width, cb_width):
    u = np.arange(tile_rows, dtype=np.float64)
    v = np.arange(width, dtype=np.float64)
    lam = (4.0 * np.sin(np.pi * u / tile_rows) ** 2)[:, None] + (4.0 * np.sin(np.pi * v / width) ** 2)[None, :]
    folded = np.minimum(v, width - v)
    ramp = ramp_gain * (folded / width) * (0.5 + 0.5 * np.cos(2.0 * np.pi * folded / width))
    taps = np.real(np.fft.ifft2(ramp[None, :] / (1.0 + paganin_beta * lam)))
    lags = tile_rows // 2 + 1
    cb_width = cb_width // SHIFTS
    place = (np.arange(cb_width)[:, None] - np.arange(width)[None, :]) % width
    table = taps[:lags][:, place].reshape(lags * cb_width, width)
    chunks = width // CHUNK
    return table.reshape(lags * cb_width, chunks, CHUNK).transpose(1, 0, 2)


def kernel(regions, tiles, starts, proj, flats, table, weights, out,
           starts_s, proj_v, flats_v, table_v, weights_v, xs, ys, sbuf, rbuf,
           load_sem, table_sem, send_sem, recv_sem):
    rows, width = flats.shape
    blocks = width // LANES
    chunks = table.shape[0]
    angles, cb, _ = weights.shape
    per = LANES // cb
    half = rows // 2
    me = lax.axis_index("ang")
    row = lax.axis_index("row")

    def peer(step, delta):
        return {"ang": lax.rem(me + step, regions), "row": lax.rem(row + delta + tiles, tiles)}

    links = [(step, delta) for step in range(regions) for delta in (-1, 0, 1) if (step, delta) != (0, 0)]

    def when_there(delta, action):
        if delta == 0:
            action()
        else:
            pl.when(row > 0 if delta < 0 else row < tiles - 1)(action)

    loads = [pltpu.make_async_copy(proj.at[0], proj_v, load_sem.at[0]),
             pltpu.make_async_copy(flats, flats_v, load_sem.at[1]),
             pltpu.make_async_copy(starts, starts_s, load_sem.at[3])]
    late = [pltpu.make_async_copy(table.at[k], table_v.at[k], table_sem.at[k]) for k in range(chunks)]
    weight_load = pltpu.make_async_copy(weights, weights_v, load_sem.at[2])
    for copy in loads + late + [weight_load]:
        copy.start()

    barrier = pltpu.get_barrier_semaphore()
    for step, delta in links:
        when_there(delta, lambda: pl.semaphore_signal(
            barrier, inc=1, device_id=peer(step, delta), device_id_type=pl.DeviceIdType.MESH))
    zeros = jnp.zeros((angles, rows, LANES), jnp.bfloat16)
    pl.when(row == tiles - 1)(lambda: rbuf.at[0].__setitem__(..., zeros))
    pl.when(row == 0)(lambda: rbuf.at[2].__setitem__(..., zeros))

    for copy in loads:
        copy.wait()

    pieces = [slice(b * LANES, (b + 1) * LANES) for b in range(blocks)]
    contrast = [1.0 - proj_v[:, p].astype(jnp.float32) / flats_v[:, p] for p in pieces]
    mean = jnp.sum(sum(contrast), axis=1, keepdims=True) / width
    for b, x in enumerate(contrast):
        xs[b] = x - mean
        xs[b + blocks] = x - mean

    lane = lax.broadcasted_iota(jnp.int32, (rows, LANES), 1)
    sub = lax.broadcasted_iota(jnp.int32, (rows, LANES), 0)
    cs = cb // SHIFTS
    for g in range(regions):
        shifted = []
        for k in range(SHIFTS):
            start = starts_s[me, g] + k * cs
            first = start // LANES
            rest = lax.rem(start, LANES)
            shift = lax.rem(LANES - rest, LANES)
            low = lane < LANES - rest
            turned = [pltpu.roll(xs[first + b], shift, 1) for b in range(blocks + 1)]
            shifted.append([jnp.where(low, turned[b], turned[b + 1]) for b in range(blocks)])
        for b in range(blocks):
            ys[g * SHIFTS * rows:(g + 1) * SHIFTS * rows, b * LANES:(b + 1) * LANES] = jnp.concatenate(
                [y[b] for y in shifted], axis=0).astype(jnp.bfloat16)

    total = None
    for k in range(chunks):
        late[k].wait()
        part = lax.dot_general(ys[:, k * CHUNK:(k + 1) * CHUNK], table_v[k], (((1,), (1,)), ((), ())),
                               preferred_element_type=jnp.float32)
        total = part if total is None else total + part

    lags = rows + 1
    pad = -(lags * cs) % LANES
    total = jnp.concatenate([total, jnp.zeros((total.shape[0], pad), jnp.float32)], axis=1)
    spot = lax.rem(me, per) * cb
    mine = (lane >= spot) & (lane < spot + cb)
    for g in range(regions):
        lag = []
        for d in range(lags):
            column = d * cs // LANES * LANES
            merged = None
            for k in range(SHIFTS):
                base = (g * SHIFTS + k) * rows
                tile = total[base:base + rows, column:column + LANES]
                tile = pltpu.roll(tile, lax.rem(spot + k * cs + LANES - d * cs % LANES, LANES), 1)
                merged = tile if k == 0 else jnp.where(lane < spot + k * cs, merged, tile)
            lag.append(merged)
        own = lag[0]
        after = jnp.where(sub >= half, lag[rows], 0.0)
        before = jnp.where(sub < half, lag[rows], 0.0)
        for e in range(1, rows):
            a = pltpu.roll(lag[e], e, 0)
            b = pltpu.roll(lag[rows - e], e, 0)
            own = own + jnp.where(sub >= e, a, b)
            other = jnp.where(sub >= e, b, a)
            source = lax.rem(sub + rows - e, rows)
            after = after + jnp.where(source >= half, other, 0.0)
            before = before + jnp.where(source < half, other, 0.0)
        sbuf[0, g] = jnp.where(mine, before, 0.0).astype(jnp.bfloat16)
        sbuf[1, g] = jnp.where(mine, own, 0.0).astype(jnp.bfloat16)
        sbuf[2, g] = jnp.where(mine, after, 0.0).astype(jnp.bfloat16)

    sides = (row > 0).astype(jnp.int32) + (row < tiles - 1).astype(jnp.int32)
    pl.semaphore_wait(barrier, regions - 1 + sides * regions)

    def message(step, delta):
        to = peer(step, delta)
        region = to["ang"]
        return pltpu.make_async_remote_copy(
            src_ref=sbuf.at[delta + 1, region], dst_ref=rbuf.at[delta + 1, me],
            send_sem=send_sem.at[delta + 1, region], recv_sem=recv_sem.at[delta + 1, me],
            device_id=to, device_id_type=pl.DeviceIdType.MESH)

    sent = [message(step, delta) for step, delta in links]
    for (step, delta), copy in zip(links, sent):
        when_there(delta, copy.start)
    weight_load.wait()

    def arrived(step, delta):
        angle = lax.rem(me + step, regions)
        copy = pltpu.make_async_remote_copy(
            src_ref=sbuf.at[delta + 1, angle], dst_ref=rbuf.at[delta + 1, angle],
            send_sem=send_sem.at[delta + 1, angle], recv_sem=recv_sem.at[delta + 1, angle],
            device_id=peer(step, delta), device_id_type=pl.DeviceIdType.MESH)
        when_there(-delta, copy.wait_recv)

    rbuf[1, me] = sbuf[1, me]
    for step, delta in links:
        arrived(step, delta)

    result = jnp.zeros(out.shape, jnp.float32)
    for group in range(-(-angles // per)):
        block = jnp.zeros((rows, LANES), jnp.float32)
        members = range(group * per, min(angles, (group + 1) * per))
        for a in members:
            block = block + rbuf[1, a].astype(jnp.float32)
            block = block + rbuf[0, a].astype(jnp.float32)
            block = block + rbuf[2, a].astype(jnp.float32)
        block = block.astype(jnp.bfloat16)
        depth = len(members) * cb
        w = weights_v[group * per:group * per + len(members)].reshape(depth, out.shape[1])
        result = result + jnp.dot(block[:, :depth], w, preferred_element_type=jnp.float32)
    out[...] = result
    for (step, delta), copy in zip(links, sent):
        when_there(delta, copy.wait_send)


def body(projections, flats, block_start, bp_weights):
    _, rows, width = projections.shape
    angles, cb, pixels = bp_weights.shape
    regions, tiles = lax.axis_size("ang"), lax.axis_size("row")
    table = jnp.asarray(filter_table(rows + 2 * HALO, width, cb), jnp.bfloat16)
    hbm = pl.BlockSpec(memory_space=pltpu.HBM)
    return pl.pallas_call(
        functools.partial(kernel, regions, tiles),
        name="fbp",
        out_shape=pltpu.VMEM((rows, pixels), jnp.float32),
        in_specs=[hbm, hbm, hbm, hbm, hbm],
        out_specs=pl.BlockSpec(memory_space=pltpu.VMEM),
        scratch_shapes=[
            pltpu.SMEM(block_start.shape, jnp.int32),
            pltpu.VMEM((rows, width), jnp.bfloat16),
            pltpu.VMEM((rows, width), jnp.float32),
            pltpu.VMEM(table.shape, jnp.bfloat16),
            pltpu.VMEM(bp_weights.shape, jnp.bfloat16),
            pltpu.VMEM((2 * width // LANES, rows, LANES), jnp.float32),
            pltpu.VMEM((regions * SHIFTS * rows, width), jnp.bfloat16),
            pltpu.VMEM((3, regions, rows, LANES), jnp.bfloat16),
            pltpu.VMEM((3, angles, rows, LANES), jnp.bfloat16),
            pltpu.SemaphoreType.DMA((4,)),
            pltpu.SemaphoreType.DMA((table.shape[0],)),
            pltpu.SemaphoreType.DMA((3, regions)),
            pltpu.SemaphoreType.DMA((3, angles)),
        ],
        compiler_params=pltpu.CompilerParams(collective_id=0, has_side_effects=True, vmem_limit_bytes=65000000),
    )(block_start, projections, flats, table, bp_weights)


def solution(mesh):
    placed = (P(("scan", "ang"), "row", None), P(("scan", "row"), None), P(), P(None, None, "ang"))
    return jax.shard_map(
        body, mesh=mesh, in_specs=placed, out_specs=P(("scan", "row"), "ang"), check_vma=False
    )
```

```python
import functools

import jax
import jax.numpy as jnp
import numpy as np
from jax import lax
from jax.experimental import pallas as pl
from jax.experimental.pallas import tpu as pltpu
from jax.sharding import PartitionSpec as P

HALO = 4
LANES = 128
SHIFTS = 2
paganin_beta = 8.0
ramp_gain = 320.0


def filter_table(tile_rows, width, cb_width):
    u = np.arange(tile_rows, dtype=np.float64)
    v = np.arange(width, dtype=np.float64)
    lam = (4.0 * np.sin(np.pi * u / tile_rows) ** 2)[:, None] + (4.0 * np.sin(np.pi * v / width) ** 2)[None, :]
    folded = np.minimum(v, width - v)
    ramp = ramp_gain * (folded / width) * (0.5 + 0.5 * np.cos(2.0 * np.pi * folded / width))
    taps = np.real(np.fft.ifft2(ramp[None, :] / (1.0 + paganin_beta * lam)))
    lags = tile_rows // 2 + 1
    cb_width = cb_width // SHIFTS
    place = (np.arange(cb_width)[:, None] - np.arange(width)[None, :]) % width
    return taps[:lags][:, place].reshape(lags * cb_width, width)


def kernel(regions, tiles, starts, proj, flats, table, weights, out,
           starts_s, proj_v, flats_v, table_v, weights_v, xs, ys, sbuf, rbuf,
           load_sem, table_sem, send_sem, recv_sem):
    rows, width = flats.shape
    blocks = width // LANES
    angles, cb, _ = weights.shape
    per = LANES // cb
    half = rows // 2
    me = lax.axis_index("ang")
    row = lax.axis_index("row")

    def peer(step, delta):
        return {"ang": lax.rem(me + step, regions), "row": lax.rem(row + delta + tiles, tiles)}

    links = [(step, delta) for step in range(regions) for delta in (-1, 0, 1) if (step, delta) != (0, 0)]

    def when_there(delta, action):
        if delta == 0:
            action()
        else:
            pl.when(row > 0 if delta < 0 else row < tiles - 1)(action)

    loads = [pltpu.make_async_copy(proj.at[0], proj_v, load_sem.at[0]),
             pltpu.make_async_copy(flats, flats_v, load_sem.at[1]),
             pltpu.make_async_copy(starts, starts_s, load_sem.at[3])]
    late = [pltpu.make_async_copy(table, table_v, table_sem)]
    weight_load = pltpu.make_async_copy(weights, weights_v, load_sem.at[2])
    for copy in loads + late + [weight_load]:
        copy.start()

    barrier = pltpu.get_barrier_semaphore()
    for step, delta in links:
        when_there(delta, lambda: pl.semaphore_signal(
            barrier, inc=1, device_id=peer(step, delta), device_id_type=pl.DeviceIdType.MESH))
    zeros = jnp.zeros((angles, rows, LANES), jnp.bfloat16)
    pl.when(row == tiles - 1)(lambda: rbuf.at[0].__setitem__(..., zeros))
    pl.when(row == 0)(lambda: rbuf.at[2].__setitem__(..., zeros))

    for copy in loads:
        copy.wait()

    pieces = [slice(b * LANES, (b + 1) * LANES) for b in range(blocks)]
    contrast = [1.0 - proj_v[:, p].astype(jnp.float32) / flats_v[:, p] for p in pieces]
    mean = jnp.sum(sum(contrast), axis=1, keepdims=True) / width
    for b, x in enumerate(contrast):
        xs[b] = x - mean
        xs[b + blocks] = x - mean

    lane = lax.broadcasted_iota(jnp.int32, (rows, LANES), 1)
    sub = lax.broadcasted_iota(jnp.int32, (rows, LANES), 0)
    cs = cb // SHIFTS
    for g in range(regions):
        shifted = []
        for k in range(SHIFTS):
            start = starts_s[me, g] + k * cs
            first = start // LANES
            rest = lax.rem(start, LANES)
            shift = lax.rem(LANES - rest, LANES)
            low = lane < LANES - rest
            turned = [pltpu.roll(xs[first + b], shift, 1) for b in range(blocks + 1)]
            shifted.append([jnp.where(low, turned[b], turned[b + 1]) for b in range(blocks)])
        for b in range(blocks):
            ys[g * SHIFTS * rows:(g + 1) * SHIFTS * rows, b * LANES:(b + 1) * LANES] = jnp.concatenate(
                [y[b] for y in shifted], axis=0).astype(jnp.bfloat16)

    late[0].wait()
    total = lax.dot_general(ys[...], table_v[...], (((1,), (1,)), ((), ())), preferred_element_type=jnp.float32)

    lags = rows + 1
    pad = -(lags * cs) % LANES
    total = jnp.concatenate([total, jnp.zeros((total.shape[0], pad), jnp.float32)], axis=1)
    spot = lax.rem(me, per) * cb
    mine = (lane >= spot) & (lane < spot + cb)
    for g in range(regions):
        lag = []
        for d in range(lags):
            column = d * cs // LANES * LANES
            merged = None
            for k in range(SHIFTS):
                base = (g * SHIFTS + k) * rows
                tile = total[base:base + rows, column:column + LANES]
                tile = pltpu.roll(tile, lax.rem(spot + k * cs + LANES - d * cs % LANES, LANES), 1)
                merged = tile if k == 0 else jnp.where(lane < spot + k * cs, merged, tile)
            lag.append(merged)
        own = lag[0]
        after = jnp.where(sub >= half, lag[rows], 0.0)
        before = jnp.where(sub < half, lag[rows], 0.0)
        for e in range(1, rows):
            a = pltpu.roll(lag[e], e, 0)
            b = pltpu.roll(lag[rows - e], e, 0)
            own = own + jnp.where(sub >= e, a, b)
            other = jnp.where(sub >= e, b, a)
            source = lax.rem(sub + rows - e, rows)
            after = after + jnp.where(source >= half, other, 0.0)
            before = before + jnp.where(source < half, other, 0.0)
        sbuf[0, g] = jnp.where(mine, before, 0.0).astype(jnp.bfloat16)
        sbuf[1, g] = jnp.where(mine, own, 0.0).astype(jnp.bfloat16)
        sbuf[2, g] = jnp.where(mine, after, 0.0).astype(jnp.bfloat16)

    sides = (row > 0).astype(jnp.int32) + (row < tiles - 1).astype(jnp.int32)
    pl.semaphore_wait(barrier, regions - 1 + sides * regions)

    def message(step, delta):
        to = peer(step, delta)
        region = to["ang"]
        return pltpu.make_async_remote_copy(
            src_ref=sbuf.at[delta + 1, region], dst_ref=rbuf.at[delta + 1, me],
            send_sem=send_sem.at[delta + 1, region], recv_sem=recv_sem.at[delta + 1, me],
            device_id=to, device_id_type=pl.DeviceIdType.MESH)

    sent = [message(step, delta) for step, delta in links]
    for (step, delta), copy in zip(links, sent):
        when_there(delta, copy.start)
    weight_load.wait()

    def arrived(step, delta):
        angle = lax.rem(me + step, regions)
        copy = pltpu.make_async_remote_copy(
            src_ref=sbuf.at[delta + 1, angle], dst_ref=rbuf.at[delta + 1, angle],
            send_sem=send_sem.at[delta + 1, angle], recv_sem=recv_sem.at[delta + 1, angle],
            device_id=peer(step, delta), device_id_type=pl.DeviceIdType.MESH)
        when_there(-delta, copy.wait_recv)

    rbuf[1, me] = sbuf[1, me]
    for step, delta in links:
        arrived(step, delta)

    result = jnp.zeros(out.shape, jnp.float32)
    for group in range(-(-angles // per)):
        block = jnp.zeros((rows, LANES), jnp.float32)
        members = range(group * per, min(angles, (group + 1) * per))
        for a in members:
            block = block + rbuf[1, a].astype(jnp.float32)
            block = block + rbuf[0, a].astype(jnp.float32)
            block = block + rbuf[2, a].astype(jnp.float32)
        block = block.astype(jnp.bfloat16)
        depth = len(members) * cb
        w = weights_v[group * per:group * per + len(members)].reshape(depth, out.shape[1])
        result = result + jnp.dot(block[:, :depth], w, preferred_element_type=jnp.float32)
    out[...] = result
    for (step, delta), copy in zip(links, sent):
        when_there(delta, copy.wait_send)


def body(projections, flats, block_start, bp_weights):
    _, rows, width = projections.shape
    angles, cb, pixels = bp_weights.shape
    regions, tiles = lax.axis_size("ang"), lax.axis_size("row")
    table = jnp.asarray(filter_table(rows + 2 * HALO, width, cb), jnp.bfloat16)
    hbm = pl.BlockSpec(memory_space=pltpu.HBM)
    return pl.pallas_call(
        functools.partial(kernel, regions, tiles),
        name="fbp",
        out_shape=pltpu.VMEM((rows, pixels), jnp.float32),
        in_specs=[hbm, hbm, hbm, hbm, hbm],
        out_specs=pl.BlockSpec(memory_space=pltpu.VMEM),
        scratch_shapes=[
            pltpu.SMEM(block_start.shape, jnp.int32),
            pltpu.VMEM((rows, width), jnp.bfloat16),
            pltpu.VMEM((rows, width), jnp.float32),
            pltpu.VMEM(table.shape, jnp.bfloat16),
            pltpu.VMEM(bp_weights.shape, jnp.bfloat16),
            pltpu.VMEM((2 * width // LANES, rows, LANES), jnp.float32),
            pltpu.VMEM((regions * SHIFTS * rows, width), jnp.bfloat16),
            pltpu.VMEM((3, regions, rows, LANES), jnp.bfloat16),
            pltpu.VMEM((3, angles, rows, LANES), jnp.bfloat16),
            pltpu.SemaphoreType.DMA((4,)),
            pltpu.SemaphoreType.DMA,
            pltpu.SemaphoreType.DMA((3, regions)),
            pltpu.SemaphoreType.DMA((3, angles)),
        ],
        compiler_params=pltpu.CompilerParams(collective_id=0, has_side_effects=True, vmem_limit_bytes=65000000),
    )(block_start, projections, flats, table, bp_weights)


def solution(mesh):
    placed = (P(("scan", "ang"), "row", None), P(("scan", "row"), None), P(), P(None, None, "ang"))
    return jax.shard_map(
        body, mesh=mesh, in_specs=placed, out_specs=P(("scan", "row"), "ang"), check_vma=False
    )
```
